32 devices in a mesh: lon: 8 (over z, x), ens: 4 (over y, core).
Axes of the slice: x: 2, y: 2, z: 4, core: 2. Of those that a mesh axis runs over, the one named last changes fastest.
Arguments:
- perturb: bfloat16 [32, 32, 4096], P(None, 'lon'), may hold values from -6 to 6
- eig_table: bfloat16 [24, 32, 4096], P(None, 'lon'), may hold values from -8 to 8
- mode_index: int32 [16], replicated, may hold values from 0 to 23, as said below
- mean_state: bfloat16 [32, 4096], P('lon'), may hold values from -6 to 6
- obs_col: int32 [65536], P('lon'), may hold values from 0 to 3
- obs_row: int32 [65536], P('lon'), may hold values from 0 to 4095
- obs_frac: float32 [65536], P('lon'), may hold values from 0 to 1
- obs_value: float32 [65536], P('lon'), may hold values from -20 to 20
- obs_sigma: float32 [65536], P('lon'), may hold values from 0.5 to 2
Outputs:
- analysis: bfloat16 [512, 32, 4096], P('ens', 'lon')
- increment: float32 [32, 4096], P('lon')
The draws below stay inside these ranges and needn't reach their ends.
Inputs may be any that keep to these rules, and one draw needn't show every extreme that they name: `mode_index`: distinct entries.
All inputs are finite; a program needn't handle non-finite values.
Results may differ from the reference program's by a relative error of at most 0.009.
Values may be sent and summed in bfloat16 or wider, within the bound.
A program may use at most 128 MiB of HBM per device.

```python
import math
import jax
import jax.numpy as jnp
from jax import lax

MEMBERS = 32
MODES = 16
TABLE = 24
NLAT = 4096
LON_DEV = 4
OBS_DEV = 8192
COLUMNS = 512
NLON = 32
NOBS = 65536
N_LON = 8


def draw_mode_index(key, part):
    return jax.random.permutation(key, TABLE)[:MODES].astype(jnp.int32)


def draw_eig_table(key, part):
    subkeys = jax.random.split(key, 3)
    own_part = jax.random.normal(subkeys[0], (TABLE, NLON, NLAT), jnp.float32)
    common = 0.7 * jax.random.normal(subkeys[2], (1, NLON, NLAT), jnp.float32)
    result = own_part + common
    return jnp.clip(result, -8.0, 8.0).astype(jnp.bfloat16)


def draw_obs_value(key, part):
    subkeys = jax.random.split(key, 3)
    noise_draw = jax.random.normal(subkeys[0], (NOBS,), jnp.float32)
    result = noise_draw
    return jnp.clip(result, -20.0, 20.0)


def set_ends(drawn, rng, low, largest):
    index_at = [jax.random.randint(jax.random.fold_in(rng, axis), (), 0, length) for axis, length in enumerate(drawn.shape)]
    longest = drawn.shape.index(max(drawn.shape))
    neighbour = index_at[:longest] + [(index_at[longest] + 1) % drawn.shape[longest]] + index_at[longest + 1:]
    return drawn.at[tuple(index_at)].set(low).at[tuple(neighbour)].set(largest)


def block_levels(key, dims, pieces, low, top_value):
    loudness, own = 1.0, jax.random.fold_in(key, 6)
    for dim, shards_of in pieces:
        heights = jnp.exp(jax.random.uniform(jax.random.fold_in(own, dim), (shards_of,), jnp.float32, low / len(pieces), top_value / len(pieces)))
        loudness = loudness * jnp.repeat(heights, dims[dim] // shards_of).reshape([-1 if axis == dim else 1 for axis in range(len(dims))])
    return loudness


def noise(key, extent, width, bound, cuts=(), kind=jnp.bfloat16):
    values = jax.random.normal(key, extent, jnp.float32) * width
    if len(cuts) > 0:
        values = block_levels(key, extent, cuts, -0.22, 0.18) * values
    return jnp.clip(values, min=-bound, max=bound).astype(kind)


def setup_inputs(seed: int = 0) -> dict:
    key_list = jax.random.split(jax.random.key(seed), 10)
    return {
        "perturb": noise(key_list[0], (MEMBERS, NLON, NLAT), 1.0, 6.0, ((1, 8),)),
        "eig_table": draw_eig_table(jax.random.fold_in(key_list[9], 71), 0),
        "mode_index": draw_mode_index(jax.random.fold_in(key_list[9], 71), 0),
        "mean_state": noise(key_list[3], (NLON, NLAT), 1.0, 6.0, ((0, 8),)),
        "obs_col": set_ends(jax.random.randint(key_list[4], (NOBS,), 0, LON_DEV), jax.random.fold_in(key_list[4], 1), 0, LON_DEV - 1).astype(jnp.int32),
        "obs_row": set_ends(jax.random.randint(key_list[5], (NOBS,), 0, NLAT), jax.random.fold_in(key_list[5], 1), 0, NLAT - 1).astype(jnp.int32),
        "obs_frac": jnp.clip(1.0 * jax.random.uniform(key_list[6], (NOBS,), jnp.float32) ** block_levels(key_list[6], (NOBS,), ((0, 8),), -0.2, 0.2), 0.0, 1.0),
        "obs_value": draw_obs_value(jax.random.fold_in(key_list[9], 71), 0),
        "obs_sigma": jnp.clip(jnp.exp(math.log(2.0) - 1.3862944 * jax.random.uniform(key_list[8], (NOBS,), jnp.float32) ** block_levels(key_list[8], (NOBS,), ((0, 8),), -0.2, 0.2)), 0.5, 2.0),
    }


def reference(perturb, eig_table, mode_index, mean_state, obs_col, obs_row, obs_frac, obs_value, obs_sigma):
    inv_root = 1.0 / jnp.sqrt(jnp.float32(MEMBERS - 1))
    obs_scale = jnp.sqrt(jnp.float32(4 * MEMBERS) / jnp.float32(NOBS))
    chosen = eig_table[mode_index].astype(jnp.float32)
    member_rows = perturb.astype(jnp.float32)
    mean_rows = mean_state.astype(jnp.float32)

    def band_terms(band_index):
        first_obs = band_index * OBS_DEV
        band_cols = lax.dynamic_slice_in_dim(obs_col, first_obs, OBS_DEV)
        band_rows = lax.dynamic_slice_in_dim(obs_row, first_obs, OBS_DEV)
        fraction = lax.dynamic_slice_in_dim(obs_frac, first_obs, OBS_DEV)
        observed = lax.dynamic_slice_in_dim(obs_value, first_obs, OBS_DEV)
        obs_error = lax.dynamic_slice_in_dim(obs_sigma, first_obs, OBS_DEV)
        lon_here = (band_index * LON_DEV + band_cols).astype(jnp.int32)
        lon_next = ((lon_here + 1) % NLON).astype(jnp.int32)
        pert_here = member_rows[:, lon_here, band_rows]
        pert_next = member_rows[:, lon_next, band_rows]
        mode_here = chosen[:, lon_here, band_rows]
        mode_next = chosen[:, lon_next, band_rows]
        blended = (1.0 - fraction) * mode_here[:, None, :] * pert_here[None] + fraction * mode_next[:, None, :] * pert_next[None]
        obs_columns = (blended * (obs_scale * inv_root / obs_error)).reshape(COLUMNS, OBS_DEV)
        normed = (observed - ((1.0 - fraction) * mean_rows[lon_here, band_rows] + fraction * mean_rows[lon_next, band_rows])) / obs_error
        rounded = obs_columns.astype(jnp.bfloat16)
        gram_part = jnp.dot(rounded.astype(jnp.float32), rounded.T.astype(jnp.float32), preferred_element_type=jnp.float32)
        gain_part = jnp.dot(obs_columns, normed, precision=lax.Precision.HIGHEST)
        return (gram_part, gain_part, jnp.sum(normed * normed))
    gram_parts, gain_parts, square_parts = lax.map(band_terms, jnp.arange(N_LON, dtype=jnp.int32))
    gram_matrix = lax.optimization_barrier(jnp.sum(gram_parts, axis=0))
    gain_vector = lax.optimization_barrier(jnp.sum(gain_parts, axis=0))
    square_sum = jnp.sum(square_parts)
    prior_scale = 2.0 / (1.0 + square_sum / NOBS)
    identity = jnp.eye(COLUMNS, dtype=jnp.float32)
    factor_lower = jnp.linalg.cholesky(identity + prior_scale * gram_matrix)
    inverse = lax.linalg.triangular_solve(factor_lower, identity, left_side=True, lower=True)
    inner = jnp.dot(inverse, gain_vector, precision=lax.Precision.HIGHEST)
    weights = jnp.sqrt(prior_scale) * jnp.dot(inverse.T, inner, precision=lax.Precision.HIGHEST)
    inverse_rounded = inverse.astype(jnp.bfloat16)
    weights_rounded = weights.astype(jnp.bfloat16)

    def band_transform(band_index):
        first_lon = band_index * LON_DEV
        band_members = lax.dynamic_slice_in_dim(member_rows, first_lon, LON_DEV, 1)
        band_modes = lax.dynamic_slice_in_dim(chosen, first_lon, LON_DEV, 1)
        columns = (band_modes[:, None] * band_members[None] * inv_root).reshape(COLUMNS, LON_DEV * NLAT).astype(jnp.bfloat16)
        increment_band = jnp.sqrt(prior_scale) * jnp.dot(weights_rounded.astype(jnp.float32), columns.astype(jnp.float32), preferred_element_type=jnp.float32)
        product = jnp.dot(inverse_rounded.astype(jnp.float32), columns.astype(jnp.float32), preferred_element_type=jnp.float32)
        analysis_band = (jnp.sqrt(prior_scale * (MEMBERS - 1)) * product).astype(jnp.bfloat16)
        return (analysis_band.reshape(COLUMNS, LON_DEV, NLAT), increment_band.reshape(LON_DEV, NLAT))
    analysis_bands, increment_bands = lax.map(band_transform, jnp.arange(N_LON, dtype=jnp.int32))
    analysis = jnp.transpose(analysis_bands, (1, 0, 2, 3)).reshape(COLUMNS, NLON, NLAT)
    increment = increment_bands.reshape(NLON, NLAT)
    return (analysis, increment)
```

```python
import functools

import jax
import jax.numpy as jnp
from jax import lax
from jax.experimental import pallas as pl
from jax.experimental.pallas import tpu as pltpu
from jax.sharding import PartitionSpec as P

HIGHEST = lax.Precision.HIGHEST
BLOCK = 128
GROUP = 8


def passed_along(value, axis, steps):
    count = lax.axis_size(axis)
    pairs = [(source, (source + steps) % count) for source in range(count)]
    return lax.ppermute(value, axis, pairs)


def inverse_factor(block):
    size = block.shape[0]
    strips = [block[8 * t : 8 * t + 8, :] for t in range(size // 8)]
    lane = lax.broadcasted_iota(jnp.int32, (8, size), 1)
    lane_row = lax.broadcasted_iota(jnp.int32, (1, size), 1)
    sub = lax.broadcasted_iota(jnp.int32, (8, size), 0)
    for first in range(0, size, GROUP):
        start = first // 8
        cols = [
            {
                t: jnp.broadcast_to(strips[t][:, first + q : first + q + 1], (8, size))
                for t in range(start, size // 8)
            }
            for q in range(GROUP)
        ]
        for q in range(GROUP):
            k = first + q
            tk, sk = k // 8, k % 8
            scale = lax.rsqrt(cols[q][tk][sk : sk + 1, :])
            row = jnp.where(lane_row == k, 1.0, strips[tk][sk : sk + 1, :]) * scale
            factors = {
                r: cols[r][tk][sk : sk + 1, :] * scale for r in range(q + 1, GROUP)
            }
            for t in range(tk, size // 8):
                below = cols[q][t] * scale
                if t == tk:
                    below = jnp.where(sub > sk, below, 0.0)
                    kept = jnp.where((lane == k) & (sub > sk), 0.0, strips[t])
                    strips[t] = jnp.where(sub == sk, row, kept - below * row)
                else:
                    strips[t] = jnp.where(lane == k, 0.0, strips[t]) - below * row
                for r in range(q + 1, GROUP):
                    cols[r][t] = cols[r][t] - below * factors[r]
    whole = jnp.concatenate(strips, axis=0)
    return jnp.where(
        lax.broadcasted_iota(jnp.int32, (size, size), 1)
        <= lax.broadcasted_iota(jnp.int32, (size, size), 0),
        whole,
        0.0,
    )


def factor_kernel(sums_ref, scale_ref, inverse_ref, weights_ref, work):
    n = work.shape[0]
    prior = scale_ref[0, 0]
    rows_at = lax.broadcasted_iota(jnp.int32, (n, n), 0)
    cols_at = lax.broadcasted_iota(jnp.int32, (n, n), 1)
    work[...] = jnp.where(rows_at == cols_at, 1.0, 0.0) + prior * sums_ref[:n, :]
    band_cols = lax.broadcasted_iota(jnp.int32, (BLOCK, n), 1)
    band_rows = lax.broadcasted_iota(jnp.int32, (BLOCK, n), 0)

    def step(i, carry):
        at = pl.multiple_of(i * BLOCK, BLOCK)
        small = inverse_factor(work[pl.ds(at, BLOCK), pl.ds(at, BLOCK)])
        band = work[pl.ds(at, BLOCK), :]
        inside = (band_cols >= at) & (band_cols < at + BLOCK)
        band = jnp.where(inside, jnp.where(band_cols - at == band_rows, 1.0, 0.0), band)
        reduced = jnp.dot(small, band, precision=HIGHEST, preferred_element_type=jnp.float32)
        ahead = jnp.where(band_cols >= at + BLOCK, reduced, 0.0)
        for piece in range(n // BLOCK):
            lo = piece * BLOCK

            @pl.when(piece > i)
            def _():
                change = lax.dot_general(
                    ahead[:, lo : lo + BLOCK],
                    reduced,
                    (((0,), (0,)), ((), ())),
                    precision=HIGHEST,
                    preferred_element_type=jnp.float32,
                )
                old = work[lo : lo + BLOCK, :]
                work[lo : lo + BLOCK, :] = jnp.where(inside, 0.0, old) - change

        work[pl.ds(at, BLOCK), :] = jnp.where(band_cols < at + BLOCK, reduced, 0.0)
        return carry

    lax.fori_loop(0, n // BLOCK, step, 0)
    inverse = work[...]
    inverse_ref[...] = inverse.astype(jnp.bfloat16)
    inner = lax.dot_general(
        sums_ref[n:, :],
        inverse,
        (((1,), (1,)), ((), ())),
        precision=HIGHEST,
        preferred_element_type=jnp.float32,
    )
    weights_ref[...] = jnp.sqrt(jnp.full((8, n), prior)) * jnp.dot(
        inner, inverse, precision=HIGHEST, preferred_element_type=jnp.float32
    )


def factor(sums, prior_scale):
    n = sums.shape[1]
    return pl.pallas_call(
        factor_kernel,
        out_shape=(
            jax.ShapeDtypeStruct((n, n), jnp.bfloat16),
            jax.ShapeDtypeStruct((8, n), jnp.float32),
        ),
        in_specs=[
            pl.BlockSpec(memory_space=pltpu.VMEM),
            pl.BlockSpec(memory_space=pltpu.SMEM),
        ],
        out_specs=(
            pl.BlockSpec(memory_space=pltpu.VMEM),
            pl.BlockSpec(memory_space=pltpu.VMEM),
        ),
        scratch_shapes=[pltpu.VMEM((n, n), jnp.float32)],
        name="factor",
    )(sums, prior_scale.reshape(1, 1))


def local(
    perturb, eig_table, mode_index, mean_state, obs_col, obs_row, obs_frac, obs_value, obs_sigma
):
    members, lon_cols, lat_cells = perturb.shape
    table_rows = eig_table.shape[0]
    mode_count = mode_index.shape[0]
    obs_local = obs_col.shape[0]
    lon_devices = lax.axis_size("lon")
    ens_devices = lax.axis_size("ens")
    ens_rank = lax.axis_index("ens")
    columns_all = mode_count * members
    own_modes = mode_count // ens_devices
    own_columns = own_modes * members
    band_cells = lon_cols * lat_cells
    inv_root = 1.0 / jnp.sqrt(jnp.float32(members - 1))
    obs_scale = jnp.sqrt(jnp.float32(4 * members) / jnp.float32(obs_local * lon_devices))
    picker = (mode_index[:, None] == jnp.arange(table_rows, dtype=jnp.int32)[None, :]).astype(
        jnp.bfloat16
    )
    chosen = jnp.dot(
        picker, eig_table.reshape(table_rows, band_cells), preferred_element_type=jnp.float32
    ).astype(jnp.bfloat16)
    edge_modes = jnp.dot(picker, eig_table[:, 0, :], preferred_element_type=jnp.float32).astype(
        jnp.bfloat16
    )
    edge_cells = jnp.concatenate([perturb[:, 0, :], edge_modes, mean_state[0:1, :]], axis=0)
    beyond = passed_along(edge_cells, "lon", -1)
    member_rows = perturb.reshape(members, band_cells)
    inner_table = jnp.concatenate(
        [member_rows, chosen, mean_state.reshape(1, band_cells)], axis=0
    )
    lookup_table = jnp.concatenate([inner_table, beyond], axis=1)

    share = obs_local // ens_devices
    first_obs = ens_rank * share

    def own(values):
        return lax.dynamic_slice_in_dim(values, first_obs, share)

    cell_here = own(obs_col) * lat_cells + own(obs_row)
    fraction, observed, obs_error = own(obs_frac), own(obs_value), own(obs_sigma)
    picked_here = jnp.take(lookup_table, cell_here, axis=1).astype(jnp.float32)
    picked_next = jnp.take(lookup_table, cell_here + lat_cells, axis=1).astype(jnp.float32)
    pert_here = picked_here[:members]
    pert_next = picked_next[:members]
    mode_here = picked_here[members : members + mode_count]
    mode_next = picked_next[members : members + mode_count]
    mean_here = picked_here[members + mode_count]
    mean_next = picked_next[members + mode_count]
    blended = (1.0 - fraction) * mode_here[:, None, :] * pert_here[None] + fraction * mode_next[
        :, None, :
    ] * pert_next[None]
    obs_columns = (blended * (obs_scale * inv_root / obs_error)).reshape(columns_all, share)
    normed = (observed - ((1.0 - fraction) * mean_here + fraction * mean_next)) / obs_error
    rounded = obs_columns.astype(jnp.bfloat16)
    gram = lax.dot_general(
        rounded, rounded, (((1,), (1,)), ((), ())), preferred_element_type=jnp.float32
    )
    gain = jnp.dot(obs_columns, normed, precision=HIGHEST)
    square = jnp.sum(normed * normed)
    tail = jnp.concatenate(
        [gain[None], jnp.full((7, columns_all), square / columns_all, jnp.float32)], axis=0
    )
    sums = lax.psum(jnp.concatenate([gram, tail], axis=0), ("lon", "ens"))
    square_sum = sums[columns_all + 1, 0] * columns_all
    prior_scale = 2.0 / (1.0 + square_sum / (obs_local * lon_devices))
    inverse, weights = factor(sums, prior_scale)

    columns = (
        (chosen.astype(jnp.float32)[:, None, :] * member_rows.astype(jnp.float32)[None] * inv_root)
        .reshape(columns_all, band_cells)
        .astype(jnp.bfloat16)
    )
    inverse_part = lax.dynamic_slice(
        inverse, (ens_rank * own_columns, 0), (own_columns, columns_all)
    )
    left = jnp.concatenate([inverse_part, weights.astype(jnp.bfloat16)], axis=0)
    product = jnp.dot(left, columns, preferred_element_type=jnp.float32)
    analysis = (
        (jnp.sqrt(prior_scale * (members - 1)) * product[:own_columns])
        .astype(jnp.bfloat16)
        .reshape(own_columns, lon_cols, lat_cells)
    )
    increment = (jnp.sqrt(prior_scale) * product[own_columns]).reshape(lon_cols, lat_cells)
    return (analysis, increment)


def solution(mesh):
    return jax.shard_map(
        local,
        mesh=mesh,
        in_specs=(
            P(None, "lon", None),
            P(None, "lon", None),
            P(),
            P("lon", None),
            P("lon"),
            P("lon"),
            P("lon"),
            P("lon"),
            P("lon"),
        ),
        out_specs=(P("ens", "lon", None), P("lon", None)),
        check_vma=False,
    )
```
